32 devices in a mesh: expert: 4 (over x, core), shard: 8 (over z, y).
Axes of the slice: x: 2, y: 2, z: 4, core: 2. Of those that a mesh axis runs over, the one named last changes fastest.
Arguments:
- master_gate: float32 [64, 2048, 1024], P('expert', 'shard'), may hold values from -0.1875 to 0.1875
- master_up: float32 [64, 2048, 1024], P('expert', 'shard'), may hold values from -0.1875 to 0.1875
- master_down: float32 [64, 1024, 2048], P('expert', None, 'shard'), may hold values from -0.25 to 0.25
- router_weight: float32 [2048, 64], P('shard', 'expert'), may hold values from -0.125 to 0.125
- router_gain: float32 [2048], P('shard'), may hold values from 0.25 to 1.75
Outputs:
- final_gate: bfloat16 [64, 2048, 1024], P('expert', None, 'shard')
- final_up: bfloat16 [64, 2048, 1024], P('expert', None, 'shard')
- final_down: bfloat16 [64, 1024, 2048], P('expert', 'shard')
- scale_gate: float32 [64, 1024], P('expert', 'shard')
- scale_up: float32 [64, 1024], P('expert', 'shard')
- scale_down: float32 [64, 1024], P('expert', 'shard')
- serve_router: bfloat16 [2048, 64], replicated
The draws below stay inside these ranges and needn't reach their ends.
All inputs are finite; a program needn't handle non-finite values.
Results may differ from the reference program's by a relative error of at most 0.001.
Values may be sent and summed in bfloat16 or wider, within the bound.
A program may use at most 192 MiB of HBM per device.

```python
import jax
import jax.numpy as jnp
from jax import lax

EXPERTS = 64
D_MODEL = 2048
D_EXPERT = 1024


def with_spikes(entries, rng, source, target, shards_of, factor):
    def block_of(axis_at):
        return (jnp.arange(entries.shape[axis_at]) // (entries.shape[axis_at] // shards_of)).reshape((-1,) + (1,) * (entries.ndim - 1 - axis_at))

    first = jax.random.permutation(rng, shards_of)[block_of(target)]
    far = (block_of(target) + shards_of // 2) % shards_of
    return jnp.where((block_of(source) == first) | (block_of(source) == far), factor * entries, entries)


def levels(stream_key, dims, split, smallest, high):
    factor_of = 1.0
    for position, parts in split:
        steps = jax.random.uniform(jax.random.fold_in(jax.random.fold_in(stream_key, 6), position), (parts,), jnp.float32, smallest / len(split), high / len(split))
        factor_of = factor_of * jnp.repeat(jnp.exp(steps), dims[position] // parts).reshape((-1,) + (1,) * (len(dims) - 1 - position))
    return factor_of


def centred(stream_key, extent, width, bound, split=(), held_as=jnp.bfloat16):
    entries = width * jax.random.normal(stream_key, extent, jnp.float32)
    if split:
        entries = entries * levels(stream_key, extent, split, -0.22, 0.18)
    return jnp.clip(entries, -bound, bound).astype(held_as)


def bell_draw_with(rng, dims, spread, reach, pieces, heavy, dtype=jnp.bfloat16):
    values = spread * jax.random.normal(rng, dims, jnp.float32)
    if pieces:
        values = values * levels(rng, dims, pieces, -0.22, 0.18)
    return jnp.clip(with_spikes(values, jax.random.fold_in(rng, 3), *heavy), -reach, reach).astype(dtype)


def setup_inputs(seed: int = 0) -> dict:
    streams_of = jax.random.split(jax.random.key(seed), 6)
    return {
        "master_gate": bell_draw_with(streams_of[0], (EXPERTS, D_MODEL, D_EXPERT), D_MODEL ** -0.5, 0.1875, ((0, 4), (1, 8)), (1, 2, 8, 2.0), jnp.float32),
        "master_up": bell_draw_with(streams_of[1], (EXPERTS, D_MODEL, D_EXPERT), D_MODEL ** -0.5, 0.1875, ((0, 4), (1, 8)), (1, 2, 8, 2.0), jnp.float32),
        "master_down": bell_draw_with(streams_of[2], (EXPERTS, D_EXPERT, D_MODEL), D_EXPERT ** -0.5, 0.25, ((0, 4), (2, 8)), (2, 1, 8, 2.0), jnp.float32),
        "router_weight": centred(streams_of[3], (D_MODEL, EXPERTS), D_MODEL ** -0.5, 0.125, ((0, 8), (1, 4)), jnp.float32),
        "router_gain": jnp.clip(1.0 + 0.15 * jax.random.normal(streams_of[4], (D_MODEL,), jnp.float32), 0.25, 1.75),
    }


def reference(master_gate, master_up, master_down, router_weight, router_gain):
    scale_gate = jnp.sqrt(lax.optimization_barrier(jnp.sum(master_gate * master_gate, axis=1)))
    final_gate = (master_gate / jnp.expand_dims(scale_gate, 1)).astype(jnp.bfloat16)
    scale_up = jnp.sqrt(lax.optimization_barrier(jnp.sum(master_up * master_up, axis=1)))
    final_up = (master_up / jnp.expand_dims(scale_up, 1)).astype(jnp.bfloat16)
    scale_down = jnp.sqrt(lax.optimization_barrier(jnp.sum(master_down * master_down, axis=2)))
    final_down = (master_down / jnp.expand_dims(scale_down, 2)).astype(jnp.bfloat16)
    serve_router = (router_weight * router_gain[:, None]).astype(jnp.bfloat16)
    return (final_gate, final_up, final_down, scale_gate, scale_up, scale_down, serve_router)
```

```python
import functools

import jax
import jax.numpy as jnp
from jax import lax
from jax.experimental import pallas as pl
from jax.experimental.pallas import tpu as pltpu
from jax.sharding import PartitionSpec as P

MESH = pl.DeviceIdType.MESH
SLOTS = 6
EARLY = (0, 1, 2, 0)


def exchange(
    n, groups, late, gate, up, down, weight, gain,
    out_gate, out_up, out_down, scale_gate, scale_up, scale_down, out_router, later,
    in_gate, in_up, in_down, send_gate, send_up, send_down, raw_wide, raw_down,
    part, arrived, mine, crossed, owned, inverse, narrow_router,
    load_sem, half_send, half_recv, cross_send, cross_recv, inv_send, inv_recv,
    big_send, big_recv, own_sem, later_sem, raw_send, raw_recv, raw_out, router_sem,
):
    experts, rows, width = gate.shape
    cols = width // n
    inner = down.shape[2]
    half = n // 2
    first_late = experts - late
    lanes = min(128, inner)
    me = lax.axis_index("shard")
    grp = lax.axis_index("expert")
    side, place = me // half, me % half

    def at(across, step):
        there = lax.rem(side + across, 2)
        q = lax.rem(place + step, half)
        return there, q, there * half + q

    order = []
    for r in range(half):
        order.append((1, r))
        if half - 1 - r > 0:
            order.append((0, half - 1 - r))

    def load(t):
        slot = lax.rem(t, SLOTS)
        return [
            pltpu.make_async_copy(src.at[t], dst.at[slot], load_sem.at[slot, i])
            for i, (src, dst) in enumerate(((gate, in_gate), (up, in_up), (down, in_down)))
        ]

    for t in range(2):
        for copy in load(t):
            copy.start()

    barrier = pltpu.get_barrier_semaphore()
    for k in range(1, n):
        pl.semaphore_signal(
            barrier, inc=1, device_id={"shard": lax.rem(me + k, n)}, device_id_type=MESH
        )
    for k in range(1, groups):
        pl.semaphore_signal(
            barrier, inc=1, device_id={"expert": lax.rem(grp + k, groups)}, device_id_type=MESH
        )

    w = weight[...]
    experts_here, depth = w.shape
    narrow_router[...] = (w * gain[...]).astype(jnp.bfloat16)
    router_rows = pl.ds(pl.multiple_of(grp * experts_here, experts_here), experts_here)

    def router_block(d):
        return out_router.at[router_rows, pl.ds(pl.multiple_of(d * depth, depth), depth)]

    row_at = pl.ds(pl.multiple_of(me * rows, rows), rows)
    col_at = pl.ds(pl.multiple_of(me * inner, inner), inner)

    def router_first(across, step, sem):
        return pltpu.make_async_remote_copy(
            src_ref=narrow_router,
            dst_ref=router_block(me),
            send_sem=router_sem.at[0],
            recv_sem=router_sem.at[sem],
            device_id={"shard": at(across, step)[2]},
            device_id_type=MESH,
        )

    router_own = pltpu.make_async_copy(narrow_router, router_block(me), router_sem.at[2])

    def router_relay(step):
        across = router_block(at(1, 0)[2])
        return pltpu.make_async_remote_copy(
            src_ref=across,
            dst_ref=across,
            send_sem=router_sem.at[0],
            recv_sem=router_sem.at[1],
            device_id={"shard": at(0, step)[2]},
            device_id_type=MESH,
        )

    def router_second(k):
        return pltpu.make_async_remote_copy(
            src_ref=out_router.at[router_rows, :],
            dst_ref=out_router.at[router_rows, :],
            send_sem=router_sem.at[3],
            recv_sem=router_sem.at[4],
            device_id={"expert": lax.rem(grp + k, groups)},
            device_id_type=MESH,
        )

    def block_of(ref, slot, d):
        return ref[slot, :, pl.ds(pl.multiple_of(d * cols, cols), cols)]

    def raw_copy(r):
        i = EARLY[r % len(EARLY)]
        d = at(1, r)[2]
        return pltpu.make_async_remote_copy(
            src_ref=(send_gate, send_up, send_down)[i].at[d],
            dst_ref=raw_down.at[r] if i == 2 else raw_wide.at[r],
            send_sem=raw_send.at[r],
            recv_sem=raw_recv.at[r],
            device_id={"shard": d},
            device_id_type=MESH,
        )

    def raw_fill(r):
        i = EARLY[r % len(EARLY)]
        d = at(1, r)[2]
        if i == 2:
            x = in_down[0, pl.ds(pl.multiple_of(d * cols, cols), cols), :]
        else:
            x = block_of((in_gate, in_up)[i], 0, d)
        (send_gate, send_up, send_down)[i][d] = x.astype(jnp.bfloat16)

    def down_factor(q, h, t):
        return jnp.broadcast_to(inverse[t, q, h, 2], (lanes, cols)).T

    def raw_out_copy(r):
        s = at(1, half - r)[2]
        i = EARLY[r % len(EARLY)]
        if i == 2:
            to = out_down.at[0, :, pl.ds(pl.multiple_of(s * inner, inner), inner)]
            return pltpu.make_async_copy(raw_down.at[r], to, raw_out.at[r])
        to = (out_gate, out_up)[i].at[0, pl.ds(pl.multiple_of(s * rows, rows), rows), :]
        return pltpu.make_async_copy(raw_wide.at[r], to, raw_out.at[r])

    def raw_scale(r):
        i = EARLY[r % len(EARLY)]
        raw_copy(r).wait_recv()
        if i == 2:
            factor = down_factor(place, side, 0)
            for c in range(0, inner, lanes):
                x = raw_down[r, :, c:c + lanes].astype(jnp.float32)
                raw_down[r, :, c:c + lanes] = (x * factor).astype(jnp.bfloat16)
        else:
            x = raw_wide[r].astype(jnp.float32)
            raw_wide[r] = (x * inverse[0, place, side, i]).astype(jnp.bfloat16)

    def sums(t):
        slot = lax.rem(t, SLOTS)
        for d in range(n):
            h, q = d // half, d % half
            for i, ref in enumerate((in_gate, in_up)):
                x = ref[slot, :, d * cols:(d + 1) * cols]
                part[t, q, h, i] = jnp.sum(x * x, axis=0, keepdims=True)
            x = in_down[slot, d * cols:(d + 1) * cols, :]
            x = x * x
            folded = x[:, :lanes]
            for c in range(lanes, inner, lanes):
                folded = folded + x[:, c:c + lanes]
            part[t, q, h, 2] = jnp.sum(folded.T, axis=0, keepdims=True)
        for k in range(1, half):
            _, q, d = at(0, k)
            pltpu.make_async_remote_copy(
                src_ref=part.at[t, q],
                dst_ref=arrived.at[t, k - 1],
                send_sem=half_send,
                recv_sem=half_recv.at[t],
                device_id={"shard": d},
                device_id_type=MESH,
            ).start()

    def cross_copy(t):
        return pltpu.make_async_remote_copy(
            src_ref=mine.at[t],
            dst_ref=crossed.at[t],
            send_sem=cross_send,
            recv_sem=cross_recv.at[t],
            device_id={"shard": at(1, 0)[2]},
            device_id_type=MESH,
        )

    def cross(t):
        pltpu.make_async_copy(arrived.at[t], arrived.at[t], half_recv.at[t]).wait()
        total = part[t, place]
        for k in range(half - 1):
            total = total + arrived[t, k]
        mine[t] = total
        cross_copy(t).start()

    def reduce(t):
        cross_copy(t).wait_recv()
        for i, out in enumerate((scale_gate, scale_up, scale_down)):
            out[pl.ds(t, 1), :] = jnp.sqrt(mine[t, side, i] + crossed[t, side, i])
        scaled = 1.0 / jnp.sqrt(mine[t] + crossed[t])
        owned[t] = scaled
        inverse[t, place] = scaled
        for k in range(1, half):
            pltpu.make_async_remote_copy(
                src_ref=owned.at[t],
                dst_ref=inverse.at[t, place],
                send_sem=inv_send,
                recv_sem=inv_recv.at[t],
                device_id={"shard": at(0, k)[2]},
                device_id_type=MESH,
            ).start()

    def finish(t, first):
        others = pl.ds(0, half - 1)
        pltpu.make_async_copy(
            inverse.at[t, others], inverse.at[t, others], inv_recv.at[t]
        ).wait()
        slot = lax.rem(t, SLOTS)
        for i, (ref, send, place_at) in enumerate((
            (in_gate, send_gate, out_gate.at[t, row_at, :]),
            (in_up, send_up, out_up.at[t, row_at, :]),
            (in_down, send_down, out_down.at[t, :, col_at]),
        )):
            waiting = None
            for across, step in order + [(0, 0)]:
                if first and across == 1 and EARLY[step % len(EARLY)] == i:
                    continue
                h, q, d = at(across, step)
                to = t * n + d
                if i == 2:
                    factor = down_factor(q, h, t)
                    for c in range(0, inner, lanes):
                        x = ref[slot, pl.ds(pl.multiple_of(d * cols, cols), cols), c:c + lanes]
                        send[to, :, c:c + lanes] = (x * factor).astype(jnp.bfloat16)
                else:
                    x = block_of(ref, slot, d)
                    send[to] = (x * inverse[t, q, h, i]).astype(jnp.bfloat16)
                if waiting is not None:
                    waiting()

                def go(across=across, step=step, d=d, to=to):
                    if (across, step) == (0, 0):
                        pltpu.make_async_copy(send.at[to], place_at, own_sem.at[i]).start()
                        return
                    copy = pltpu.make_async_remote_copy(
                        src_ref=send.at[to],
                        dst_ref=place_at,
                        send_sem=big_send.at[i],
                        recv_sem=big_recv.at[i],
                        device_id={"shard": d},
                        device_id_type=MESH,
                    )
                    if i == 2 and (across, step) == (1, 0) and not first:
                        @pl.when(t < first_late)
                        def _():
                            copy.start()

                        @pl.when(t >= first_late)
                        def _():
                            pltpu.make_async_copy(
                                send.at[to], later.at[t - first_late], later_sem
                            ).start()
                    else:
                        copy.start()

                waiting = go
            waiting()

    def step(t, carry):
        @pl.when(t + 2 < experts)
        def _():
            for copy in load(t + 2):
                copy.start()

        @pl.when(t < experts)
        def _():
            for copy in load(t):
                copy.wait()
            sums(t)

        @pl.when((t >= 1) & (t <= experts))
        def _():
            cross(t - 1)

        @pl.when(t == 2)
        def _():
            for r in range(half // 2, half):
                raw_copy(r).start()

        @pl.when((t >= 2) & (t <= experts + 1))
        def _():
            reduce(t - 2)

        @pl.when(t == 3)
        def _():
            router_first(1, 0, 5).wait_recv()
            for k in range(1, half):
                router_relay(k).start()
            finish(0, True)
            for r in range(half):
                raw_scale(r)
                if r:
                    raw_out_copy(r - 1).start()
            raw_out_copy(half - 1).start()

        @pl.when(t > 3)
        def _():
            finish(t - 3, False)

        return carry

    for copy in load(2):
        copy.start()
    for copy in load(0):
        copy.wait()
    for r in range(half):
        raw_fill(r)
    pl.semaphore_wait(barrier, n - 1 + groups - 1)
    sums(0)
    router_own.start()
    for k in range(1, half):
        router_first(0, k, 1).start()
    router_first(1, 0, 5).start()
    for r in range(half // 2):
        raw_copy(r).start()
    lax.fori_loop(1, experts + 3, step, 0)

    gathered = out_router.at[router_rows, pl.ds(0, (n - 1) * depth)]
    near = out_router.at[router_rows, pl.ds(0, (n - 2) * depth)]
    router_own.wait()
    pltpu.make_async_copy(near, near, router_sem.at[1]).wait()
    for k in range(1, groups):
        router_second(k).start()

    pltpu.make_async_copy(later, later, later_sem).wait()
    for r in range(half):
        raw_copy(r).wait_send()
        raw_out_copy(r).wait()
    for i, send in enumerate((send_gate, send_up, send_down)):
        sent = experts * (n - 1) - sum(EARLY[r % len(EARLY)] == i for r in range(half))
        if i == 2:
            sent -= late
        blocks = send.at[pl.ds(0, sent)]
        pltpu.make_async_copy(blocks, blocks, big_recv.at[i]).wait()
        pltpu.make_async_copy(blocks, blocks, big_send.at[i]).wait()
        kept = send.at[pl.ds(0, experts)]
        pltpu.make_async_copy(kept, kept, own_sem.at[i]).wait()
    pltpu.make_async_copy(arrived, arrived, half_send).wait()
    pltpu.make_async_copy(crossed, crossed, cross_send).wait()
    others = pl.ds(0, half - 1)
    pltpu.make_async_copy(inverse.at[:, others], inverse.at[:, others], inv_send).wait()
    pltpu.make_async_copy(gathered, gathered, router_sem.at[0]).wait()
    handed = out_router.at[pl.ds(0, (groups - 1) * experts_here), :]
    pltpu.make_async_copy(handed, handed, router_sem.at[3]).wait()
    pltpu.make_async_copy(handed, handed, router_sem.at[4]).wait()


def by_collectives(master_gate, master_up, master_down, router_weight, router_gain):
    total_gate, total_up, total_down = lax.psum(
        (
            jnp.sum(master_gate * master_gate, axis=1),
            jnp.sum(master_up * master_up, axis=1),
            jnp.sum(master_down * master_down, axis=2),
        ),
        "shard",
    )
    scale_gate = jnp.sqrt(total_gate)
    scale_up = jnp.sqrt(total_up)
    scale_down = jnp.sqrt(total_down)
    narrow_gate, narrow_up, narrow_down = (
        (master_gate / jnp.expand_dims(scale_gate, 1)).astype(jnp.bfloat16),
        (master_up / jnp.expand_dims(scale_up, 1)).astype(jnp.bfloat16),
        (master_down / jnp.expand_dims(scale_down, 2)).astype(jnp.bfloat16),
    )
    final_gate, final_up = (
        lax.all_to_all(narrow_gate, "shard", split_axis=2, concat_axis=1, tiled=True),
        lax.all_to_all(narrow_up, "shard", split_axis=2, concat_axis=1, tiled=True),
    )
    final_down = lax.all_to_all(narrow_down, "shard", split_axis=1, concat_axis=2, tiled=True)
    scale_gate = lax.dynamic_slice_in_dim(
        scale_gate, lax.axis_index("shard") * final_gate.shape[2], final_gate.shape[2], axis=1
    )
    scale_up = lax.dynamic_slice_in_dim(
        scale_up, lax.axis_index("shard") * final_up.shape[2], final_up.shape[2], axis=1
    )
    scale_down = lax.dynamic_slice_in_dim(
        scale_down, lax.axis_index("shard") * final_down.shape[1], final_down.shape[1], axis=1
    )
    part_router = (router_weight * router_gain[:, None]).astype(jnp.bfloat16)
    row_router = lax.all_gather(part_router, "shard", axis=0, tiled=True)
    serve_router = lax.all_gather(row_router, "expert", axis=1, tiled=True)
    return (final_gate, final_up, final_down, scale_gate, scale_up, scale_down, serve_router)


def on_device(n, groups, gate, up, down, router_weight, router_gain):
    experts, rows, width = gate.shape
    cols = width // n
    inner = down.shape[2]
    depth, experts_here = router_weight.shape
    if cols % 128 or inner % 128 or depth % 128 or n % 2 or n < 4 or experts < 8:
        return by_collectives(gate, up, down, router_weight, router_gain)
    narrow, wide = jnp.bfloat16, jnp.float32
    half = n // 2
    late = experts // 2
    dma = pltpu.SemaphoreType.DMA
    any_space = pl.BlockSpec(memory_space=pl.ANY)
    vmem = pl.BlockSpec(memory_space=pltpu.VMEM)
    outs = pl.pallas_call(
        functools.partial(exchange, n, groups, late),
        out_shape=(
            jax.ShapeDtypeStruct((experts, rows * n, cols), narrow),
            jax.ShapeDtypeStruct((experts, rows * n, cols), narrow),
            jax.ShapeDtypeStruct((experts, cols, inner * n), narrow),
            jax.ShapeDtypeStruct((experts, cols), wide),
            jax.ShapeDtypeStruct((experts, cols), wide),
            jax.ShapeDtypeStruct((experts, cols), wide),
            jax.ShapeDtypeStruct((experts_here * groups, depth * n), narrow),
            jax.ShapeDtypeStruct((late, cols, inner), narrow),
        ),
        in_specs=[any_space] * 3 + [vmem] * 2,
        out_specs=(any_space,) * 3 + (vmem,) * 3 + (any_space,) * 2,
        scratch_shapes=[
            pltpu.VMEM((SLOTS, rows, width), wide),
            pltpu.VMEM((SLOTS, rows, width), wide),
            pltpu.VMEM((SLOTS, width, inner), wide),
            pltpu.VMEM((experts * n, rows, cols), narrow),
            pltpu.VMEM((experts * n, rows, cols), narrow),
            pltpu.VMEM((experts * n, cols, inner), narrow),
            pltpu.VMEM((half, rows, cols), narrow),
            pltpu.VMEM((half, cols, inner), narrow),
            pltpu.VMEM((experts, half, 2, 3, 1, cols), wide),
            pltpu.VMEM((experts, half - 1, 2, 3, 1, cols), wide),
            pltpu.VMEM((experts, 2, 3, 1, cols), wide),
            pltpu.VMEM((experts, 2, 3, 1, cols), wide),
            pltpu.VMEM((experts, 2, 3, 1, cols), wide),
            pltpu.VMEM((experts, half, 2, 3, 1, cols), wide),
            pltpu.VMEM((experts_here, depth), narrow),
            dma((SLOTS, 3)),
            dma,
            dma((experts,)),
            dma,
            dma((experts,)),
            dma,
            dma((experts,)),
            dma((3,)),
            dma((3,)),
            dma((3,)),
            dma,
            dma((half,)),
            dma((half,)),
            dma((half,)),
            dma((6,)),
        ],
        compiler_params=pltpu.CompilerParams(
            collective_id=0, has_side_effects=True, vmem_limit_bytes=60 * 2**20
        ),
    )(gate, up, down, router_weight.T, router_gain[None, :])
    swap = [(d, (d + half) % n) for d in range(n)]
    late_blocks = lax.ppermute(outs[7], "shard", swap)

    def one(shape):
        return pl.BlockSpec((1,) + shape[1:], lambda t: (t, 0, 0))

    specs = [one(x.shape) for x in outs[:3]]
    specs += [pl.BlockSpec(x.shape, lambda t: (0, 0)) for x in outs[3:7]]
    moved = sum(x.size * x.dtype.itemsize for x in outs[:7])
    placed = pl.pallas_call(
        place,
        grid=(experts,),
        in_specs=specs,
        out_specs=specs,
        out_shape=tuple(jax.ShapeDtypeStruct(x.shape, x.dtype) for x in outs[:7]),
        compiler_params=pltpu.CompilerParams(dimension_semantics=("arbitrary",)),
        cost_estimate=pl.CostEstimate(flops=0, bytes_accessed=2 * moved, transcendentals=0),
    )(*outs[:7])
    final_down = pl.pallas_call(
        functools.partial(place_late, n),
        in_specs=[any_space] * 2,
        out_specs=any_space,
        out_shape=jax.ShapeDtypeStruct(outs[2].shape, narrow),
        input_output_aliases={0: 0},
        scratch_shapes=[dma],
        compiler_params=pltpu.CompilerParams(vmem_limit_bytes=2**20),
    )(placed[2], late_blocks)
    return placed[:2] + (final_down,) + placed[3:6] + (placed[6].T,)


def place(*refs):
    half = len(refs) // 2
    for src, dst in zip(refs[:half], refs[half:]):
        dst[...] = src[...]


def place_late(n, _, late, out, sem):
    count, _, inner = late.shape
    source = lax.rem(lax.axis_index("shard") + n // 2, n)
    cols = pl.ds(pl.multiple_of(source * inner, inner), inner)
    copy = pltpu.make_async_copy(
        late, out.at[pl.ds(out.shape[0] - count, count), :, cols], sem
    )
    copy.start()
    copy.wait()


def solution(mesh):
    placed = (
        P("expert", "shard", None),
        P("expert", "shard", None),
        P("expert", None, "shard"),
        P("shard", "expert"),
        P("shard"),
    )
    return jax.shard_map(
        functools.partial(on_device, mesh.shape["shard"], mesh.shape["expert"]),
        mesh=mesh,
        in_specs=placed,
        out_specs=(
            P("expert", None, "shard"),
            P("expert", None, "shard"),
            P("expert", "shard", None),
            P("expert", "shard"),
            P("expert", "shard"),
            P("expert", "shard"),
            P(),
        ),
        check_vma=False,
    )
```

```python
import functools

import jax
import jax.numpy as jnp
from jax import lax
from jax.experimental import pallas as pl
from jax.experimental.pallas import tpu as pltpu
from jax.sharding import PartitionSpec as P

MESH = pl.DeviceIdType.MESH
SLOTS = 6
EARLY = (0, 1, 2, 0)


def exchange(
    n, groups, late, gate, up, down, weight, gain,
    out_gate, out_up, out_down, scale_gate, scale_up, scale_down, out_router, later,
    in_gate, in_up, in_down, send_gate, send_up, send_down, raw_wide, raw_down,
    part, arrived, mine, crossed, owned, inverse, narrow_router,
    load_sem, half_send, half_recv, cross_send, cross_recv, inv_send, inv_recv,
    big_send, big_recv, own_sem, later_sem, raw_send, raw_recv, raw_out, router_sem,
):
    experts, rows, width = gate.shape
    cols = width // n
    inner = down.shape[2]
    half = n // 2
    first_late = experts - late
    lanes = min(128, inner)
    me = lax.axis_index("shard")
    grp = lax.axis_index("expert")
    side, place = me // half, me % half

    def at(across, step):
        there = lax.rem(side + across, 2)
        q = lax.rem(place + step, half)
        return there, q, there * half + q

    order = []
    for r in range(half):
        order.append((1, r))
        if half - 1 - r > 0:
            order.append((0, half - 1 - r))

    def load(t):
        slot = lax.rem(t, SLOTS)
        return [
            pltpu.make_async_copy(src.at[t], dst.at[slot], load_sem.at[slot, i])
            for i, (src, dst) in enumerate(((gate, in_gate), (up, in_up), (down, in_down)))
        ]

    for t in range(2):
        for copy in load(t):
            copy.start()

    barrier = pltpu.get_barrier_semaphore()
    for k in range(1, n):
        pl.semaphore_signal(
            barrier, inc=1, device_id={"shard": lax.rem(me + k, n)}, device_id_type=MESH
        )
    for k in range(1, groups):
        pl.semaphore_signal(
            barrier, inc=1, device_id={"expert": lax.rem(grp + k, groups)}, device_id_type=MESH
        )

    w = weight[...]
    experts_here, depth = w.shape
    narrow_router[...] = (w * gain[...]).astype(jnp.bfloat16)
    router_rows = pl.ds(pl.multiple_of(grp * experts_here, experts_here), experts_here)

    def router_block(d):
        return out_router.at[router_rows, pl.ds(pl.multiple_of(d * depth, depth), depth)]

    row_at = pl.ds(pl.multiple_of(me * rows, rows), rows)
    col_at = pl.ds(pl.multiple_of(me * inner, inner), inner)

    def router_first(across, step, sem):
        return pltpu.make_async_remote_copy(
            src_ref=narrow_router,
            dst_ref=router_block(me),
            send_sem=router_sem.at[0],
            recv_sem=router_sem.at[sem],
            device_id={"shard": at(across, step)[2]},
            device_id_type=MESH,
        )

    router_own = pltpu.make_async_copy(narrow_router, router_block(me), router_sem.at[2])

    def router_relay(step):
        across = router_block(at(1, 0)[2])
        return pltpu.make_async_remote_copy(
            src_ref=across,
            dst_ref=across,
            send_sem=router_sem.at[0],
            recv_sem=router_sem.at[1],
            device_id={"shard": at(0, step)[2]},
            device_id_type=MESH,
        )

    def router_second(k):
        return pltpu.make_async_remote_copy(
            src_ref=out_router.at[router_rows, :],
            dst_ref=out_router.at[router_rows, :],
            send_sem=router_sem.at[3],
            recv_sem=router_sem.at[4],
            device_id={"expert": lax.rem(grp + k, groups)},
            device_id_type=MESH,
        )

    def block_of(ref, slot, d):
        return ref[slot, :, pl.ds(pl.multiple_of(d * cols, cols), cols)]

    def raw_copy(r):
        i = EARLY[r % len(EARLY)]
        d = at(1, r)[2]
        return pltpu.make_async_remote_copy(
            src_ref=(send_gate, send_up, send_down)[i].at[d],
            dst_ref=raw_down.at[r] if i == 2 else raw_wide.at[r],
            send_sem=raw_send.at[r],
            recv_sem=raw_recv.at[r],
            device_id={"shard": d},
            device_id_type=MESH,
        )

    def raw_fill(r):
        i = EARLY[r % len(EARLY)]
        d = at(1, r)[2]
        if i == 2:
            x = in_down[0, pl.ds(pl.multiple_of(d * cols, cols), cols), :]
        else:
            x = block_of((in_gate, in_up)[i], 0, d)
        (send_gate, send_up, send_down)[i][d] = x.astype(jnp.bfloat16)

    def down_factor(q, h, t):
        return jnp.broadcast_to(inverse[t, q, h, 2], (lanes, cols)).T

    def raw_out_copy(r):
        s = at(1, half - r)[2]
        i = EARLY[r % len(EARLY)]
        if i == 2:
            to = out_down.at[0, :, pl.ds(pl.multiple_of(s * inner, inner), inner)]
            return pltpu.make_async_copy(raw_down.at[r], to, raw_out.at[r])
        to = (out_gate, out_up)[i].at[0, pl.ds(pl.multiple_of(s * rows, rows), rows), :]
        return pltpu.make_async_copy(raw_wide.at[r], to, raw_out.at[r])

    def raw_scale(r):
        i = EARLY[r % len(EARLY)]
        raw_copy(r).wait_recv()
        if i == 2:
            factor = down_factor(place, side, 0)
            for c in range(0, inner, lanes):
                x = raw_down[r, :, c:c + lanes].astype(jnp.float32)
                raw_down[r, :, c:c + lanes] = (x * factor).astype(jnp.bfloat16)
        else:
            x = raw_wide[r].astype(jnp.float32)
            raw_wide[r] = (x * inverse[0, place, side, i]).astype(jnp.bfloat16)

    def sums(t):
        slot = lax.rem(t, SLOTS)
        for d in range(n):
            h, q = d // half, d % half
            for i, ref in enumerate((in_gate, in_up)):
                x = ref[slot, :, d * cols:(d + 1) * cols]
                part[t, q, h, i] = jnp.sum(x * x, axis=0, keepdims=True)
            x = in_down[slot, d * cols:(d + 1) * cols, :]
            x = x * x
            folded = x[:, :lanes]
            for c in range(lanes, inner, lanes):
                folded = folded + x[:, c:c + lanes]
            part[t, q, h, 2] = jnp.sum(folded.T, axis=0, keepdims=True)

    def share(t):
        for k in range(1, half):
            _, q, d = at(0, k)
            pltpu.make_async_remote_copy(
                src_ref=part.at[t, q],
                dst_ref=arrived.at[t, k - 1],
                send_sem=half_send,
                recv_sem=half_recv.at[t],
                device_id={"shard": d},
                device_id_type=MESH,
            ).start()

    def cross_copy(t):
        return pltpu.make_async_remote_copy(
            src_ref=mine.at[t],
            dst_ref=crossed.at[t],
            send_sem=cross_send,
            recv_sem=cross_recv.at[t],
            device_id={"shard": at(1, 0)[2]},
            device_id_type=MESH,
        )

    def cross(t):
        pltpu.make_async_copy(arrived.at[t], arrived.at[t], half_recv.at[t]).wait()
        total = part[t, place]
        for k in range(half - 1):
            total = total + arrived[t, k]
        mine[t] = total
        cross_copy(t).start()

    def reduce(t):
        cross_copy(t).wait_recv()
        for i, out in enumerate((scale_gate, scale_up, scale_down)):
            out[pl.ds(t, 1), :] = jnp.sqrt(mine[t, side, i] + crossed[t, side, i])
        scaled = 1.0 / jnp.sqrt(mine[t] + crossed[t])
        owned[t] = scaled
        inverse[t, place] = scaled
        for k in range(1, half):
            pltpu.make_async_remote_copy(
                src_ref=owned.at[t],
                dst_ref=inverse.at[t, place],
                send_sem=inv_send,
                recv_sem=inv_recv.at[t],
                device_id={"shard": at(0, k)[2]},
                device_id_type=MESH,
            ).start()

    def finish(t, first):
        others = pl.ds(0, half - 1)
        pltpu.make_async_copy(
            inverse.at[t, others], inverse.at[t, others], inv_recv.at[t]
        ).wait()
        slot = lax.rem(t, SLOTS)
        for i, (ref, send, place_at) in enumerate((
            (in_gate, send_gate, out_gate.at[t, row_at, :]),
            (in_up, send_up, out_up.at[t, row_at, :]),
            (in_down, send_down, out_down.at[t, :, col_at]),
        )):
            waiting = None
            for across, step in order + [(0, 0)]:
                if first and across == 1 and EARLY[step % len(EARLY)] == i:
                    continue
                h, q, d = at(across, step)
                to = t * n + d
                if i == 2:
                    factor = down_factor(q, h, t)
                    for c in range(0, inner, lanes):
                        x = ref[slot, pl.ds(pl.multiple_of(d * cols, cols), cols), c:c + lanes]
                        send[to, :, c:c + lanes] = (x * factor).astype(jnp.bfloat16)
                else:
                    x = block_of(ref, slot, d)
                    send[to] = (x * inverse[t, q, h, i]).astype(jnp.bfloat16)
                if waiting is not None:
                    waiting()

                def go(across=across, step=step, d=d, to=to):
                    if (across, step) == (0, 0):
                        pltpu.make_async_copy(send.at[to], place_at, own_sem.at[i]).start()
                        return
                    copy = pltpu.make_async_remote_copy(
                        src_ref=send.at[to],
                        dst_ref=place_at,
                        send_sem=big_send.at[i],
                        recv_sem=big_recv.at[i],
                        device_id={"shard": d},
                        device_id_type=MESH,
                    )
                    if i == 2 and (across, step) == (1, half // 2) and not first:
                        @pl.when(t < first_late)
                        def _():
                            copy.start()

                        @pl.when(t >= first_late)
                        def _():
                            pltpu.make_async_copy(
                                send.at[to], later.at[t - first_late], later_sem
                            ).start()
                    else:
                        copy.start()

                waiting = go
            waiting()

    def step(t, carry):
        @pl.when(t + 2 < experts)
        def _():
            for copy in load(t + 2):
                copy.start()

        @pl.when(t < experts)
        def _():
            for copy in load(t):
                copy.wait()
            sums(t)
            share(t)

        @pl.when((t >= 1) & (t <= experts))
        def _():
            cross(t - 1)

        @pl.when(t == 2)
        def _():
            for r in range(half // 2, half):
                raw_copy(r).start()

        @pl.when((t >= 2) & (t <= experts + 1))
        def _():
            reduce(t - 2)

        @pl.when(t == 3)
        def _():
            router_first(1, 0, 5).wait_recv()
            for k in range(1, half):
                router_relay(k).start()
            finish(0, True)
            for r in range(half):
                raw_scale(r)
                if r:
                    raw_out_copy(r - 1).start()
            raw_out_copy(half - 1).start()

        @pl.when(t > 3)
        def _():
            finish(t - 3, False)

        return carry

    for copy in load(2):
        copy.start()
    for copy in load(0):
        copy.wait()
    for r in range(half):
        raw_fill(r)
    sums(0)
    pl.semaphore_wait(barrier, n - 1 + groups - 1)
    share(0)
    router_own.start()
    for k in range(1, half):
        router_first(0, k, 1).start()
    router_first(1, 0, 5).start()
    for r in range(half // 2):
        raw_copy(r).start()
    lax.fori_loop(1, experts + 3, step, 0)

    gathered = out_router.at[router_rows, pl.ds(0, (n - 1) * depth)]
    near = out_router.at[router_rows, pl.ds(0, (n - 2) * depth)]
    router_own.wait()
    pltpu.make_async_copy(near, near, router_sem.at[1]).wait()
    for k in range(1, groups):
        router_second(k).start()

    pltpu.make_async_copy(later, later, later_sem).wait()
    for r in range(half):
        raw_copy(r).wait_send()
        raw_out_copy(r).wait()
    for i, send in enumerate((send_gate, send_up, send_down)):
        sent = experts * (n - 1) - sum(EARLY[r % len(EARLY)] == i for r in range(half))
        if i == 2:
            sent -= late
        blocks = send.at[pl.ds(0, sent)]
        pltpu.make_async_copy(blocks, blocks, big_recv.at[i]).wait()
        pltpu.make_async_copy(blocks, blocks, big_send.at[i]).wait()
        kept = send.at[pl.ds(0, experts)]
        pltpu.make_async_copy(kept, kept, own_sem.at[i]).wait()
    pltpu.make_async_copy(arrived, arrived, half_send).wait()
    pltpu.make_async_copy(crossed, crossed, cross_send).wait()
    others = pl.ds(0, half - 1)
    pltpu.make_async_copy(inverse.at[:, others], inverse.at[:, others], inv_send).wait()
    pltpu.make_async_copy(gathered, gathered, router_sem.at[0]).wait()
    handed = out_router.at[pl.ds(0, (groups - 1) * experts_here), :]
    pltpu.make_async_copy(handed, handed, router_sem.at[3]).wait()
    pltpu.make_async_copy(handed, handed, router_sem.at[4]).wait()


def by_collectives(master_gate, master_up, master_down, router_weight, router_gain):
    total_gate, total_up, total_down = lax.psum(
        (
            jnp.sum(master_gate * master_gate, axis=1),
            jnp.sum(master_up * master_up, axis=1),
            jnp.sum(master_down * master_down, axis=2),
        ),
        "shard",
    )
    scale_gate = jnp.sqrt(total_gate)
    scale_up = jnp.sqrt(total_up)
    scale_down = jnp.sqrt(total_down)
    narrow_gate, narrow_up, narrow_down = (
        (master_gate / jnp.expand_dims(scale_gate, 1)).astype(jnp.bfloat16),
        (master_up / jnp.expand_dims(scale_up, 1)).astype(jnp.bfloat16),
        (master_down / jnp.expand_dims(scale_down, 2)).astype(jnp.bfloat16),
    )
    final_gate, final_up = (
        lax.all_to_all(narrow_gate, "shard", split_axis=2, concat_axis=1, tiled=True),
        lax.all_to_all(narrow_up, "shard", split_axis=2, concat_axis=1, tiled=True),
    )
    final_down = lax.all_to_all(narrow_down, "shard", split_axis=1, concat_axis=2, tiled=True)
    scale_gate = lax.dynamic_slice_in_dim(
        scale_gate, lax.axis_index("shard") * final_gate.shape[2], final_gate.shape[2], axis=1
    )
    scale_up = lax.dynamic_slice_in_dim(
        scale_up, lax.axis_index("shard") * final_up.shape[2], final_up.shape[2], axis=1
    )
    scale_down = lax.dynamic_slice_in_dim(
        scale_down, lax.axis_index("shard") * final_down.shape[1], final_down.shape[1], axis=1
    )
    part_router = (router_weight * router_gain[:, None]).astype(jnp.bfloat16)
    row_router = lax.all_gather(part_router, "shard", axis=0, tiled=True)
    serve_router = lax.all_gather(row_router, "expert", axis=1, tiled=True)
    return (final_gate, final_up, final_down, scale_gate, scale_up, scale_down, serve_router)


def on_device(n, groups, gate, up, down, router_weight, router_gain):
    experts, rows, width = gate.shape
    cols = width // n
    inner = down.shape[2]
    depth, experts_here = router_weight.shape
    if cols % 128 or inner % 128 or depth % 128 or n % 2 or n < 4 or experts < 8:
        return by_collectives(gate, up, down, router_weight, router_gain)
    narrow, wide = jnp.bfloat16, jnp.float32
    half = n // 2
    late = experts * 8 // 16
    dma = pltpu.SemaphoreType.DMA
    any_space = pl.BlockSpec(memory_space=pl.ANY)
    vmem = pl.BlockSpec(memory_space=pltpu.VMEM)
    outs = pl.pallas_call(
        functools.partial(exchange, n, groups, late),
        out_shape=(
            jax.ShapeDtypeStruct((experts, rows * n, cols), narrow),
            jax.ShapeDtypeStruct((experts, rows * n, cols), narrow),
            jax.ShapeDtypeStruct((experts, cols, inner * n), narrow),
            jax.ShapeDtypeStruct((experts, cols), wide),
            jax.ShapeDtypeStruct((experts, cols), wide),
            jax.ShapeDtypeStruct((experts, cols), wide),
            jax.ShapeDtypeStruct((experts_here * groups, depth * n), narrow),
            jax.ShapeDtypeStruct((late, cols, inner), narrow),
        ),
        in_specs=[any_space] * 3 + [vmem] * 2,
        out_specs=(any_space,) * 3 + (vmem,) * 3 + (any_space,) * 2,
        scratch_shapes=[
            pltpu.VMEM((SLOTS, rows, width), wide),
            pltpu.VMEM((SLOTS, rows, width), wide),
            pltpu.VMEM((SLOTS, width, inner), wide),
            pltpu.VMEM((experts * n, rows, cols), narrow),
            pltpu.VMEM((experts * n, rows, cols), narrow),
            pltpu.VMEM((experts * n, cols, inner), narrow),
            pltpu.VMEM((half, rows, cols), narrow),
            pltpu.VMEM((half, cols, inner), narrow),
            pltpu.VMEM((experts, half, 2, 3, 1, cols), wide),
            pltpu.VMEM((experts, half - 1, 2, 3, 1, cols), wide),
            pltpu.VMEM((experts, 2, 3, 1, cols), wide),
            pltpu.VMEM((experts, 2, 3, 1, cols), wide),
            pltpu.VMEM((experts, 2, 3, 1, cols), wide),
            pltpu.VMEM((experts, half, 2, 3, 1, cols), wide),
            pltpu.VMEM((experts_here, depth), narrow),
            dma((SLOTS, 3)),
            dma,
            dma((experts,)),
            dma,
            dma((experts,)),
            dma,
            dma((experts,)),
            dma((3,)),
            dma((3,)),
            dma((3,)),
            dma,
            dma((half,)),
            dma((half,)),
            dma((half,)),
            dma((6,)),
        ],
        compiler_params=pltpu.CompilerParams(
            collective_id=0, has_side_effects=True, vmem_limit_bytes=60 * 2**20
        ),
    )(gate, up, down, router_weight.T, router_gain[None, :])
    swap = [(d, n - half * (d // half + 1) + (d + half // 2) % half) for d in range(n)]
    late_blocks = lax.ppermute(outs[7], "shard", swap)

    big = [jax.ShapeDtypeStruct(x.shape, x.dtype) for x in outs[:3]]
    small = [jax.ShapeDtypeStruct(x.shape, x.dtype) for x in outs[3:7]]
    moved = sum(x.size * x.dtype.itemsize for x in outs[:7])
    placed = pl.pallas_call(
        place,
        in_specs=[any_space] * 3 + [vmem] * 4,
        out_specs=[any_space] * 3 + [vmem] * 4,
        out_shape=big + small,
        scratch_shapes=[pltpu.VMEM(x.shape, x.dtype) for x in big]
        + [dma((3, experts)), dma((3, experts))],
        compiler_params=pltpu.CompilerParams(vmem_limit_bytes=60 * 2**20),
        cost_estimate=pl.CostEstimate(flops=0, bytes_accessed=2 * moved, transcendentals=0),
    )(*outs[:7])
    final_down = pl.pallas_call(
        functools.partial(place_late, n),
        in_specs=[any_space] * 2,
        out_specs=any_space,
        out_shape=jax.ShapeDtypeStruct(outs[2].shape, narrow),
        input_output_aliases={0: 0},
        scratch_shapes=[dma],
        compiler_params=pltpu.CompilerParams(vmem_limit_bytes=2**20),
    )(placed[2], late_blocks)
    return tuple(placed[:2]) + (final_down,) + tuple(placed[3:6]) + (placed[6].T,)


def place(*refs):
    srcs, dsts, held, taken, given = refs[:7], refs[7:14], refs[14:17], refs[17], refs[18]
    pairs = [(t, i) for t in range(srcs[0].shape[0]) for i in range(3)]

    def take(t, i):
        return pltpu.make_async_copy(srcs[i].at[t], held[i].at[t], taken.at[i, t])

    def give(t, i):
        return pltpu.make_async_copy(held[i].at[t], dsts[i].at[t], given.at[i, t])

    for t, i in pairs:
        take(t, i).start()
    for src, dst in zip(srcs[3:], dsts[3:]):
        dst[...] = src[...]
    for t, i in pairs:
        take(t, i).wait()
        give(t, i).start()
    for t, i in pairs:
        give(t, i).wait()


def place_late(n, _, late, out, sem):
    count, _, inner = late.shape
    me, half = lax.axis_index("shard"), n // 2
    source = (1 - me // half) * half + lax.rem(me + half // 2, half)
    cols = pl.ds(pl.multiple_of(source * inner, inner), inner)
    copy = pltpu.make_async_copy(
        late, out.at[pl.ds(out.shape[0] - count, count), :, cols], sem
    )
    copy.start()
    copy.wait()


def solution(mesh):
    placed = (
        P("expert", "shard", None),
        P("expert", "shard", None),
        P("expert", None, "shard"),
        P("shard", "expert"),
        P("shard"),
    )
    return jax.shard_map(
        functools.partial(on_device, mesh.shape["shard"], mesh.shape["expert"]),
        mesh=mesh,
        in_specs=placed,
        out_specs=(
            P("expert", None, "shard"),
            P("expert", None, "shard"),
            P("expert", "shard", None),
            P("expert", "shard"),
            P("expert", "shard"),
            P("expert", "shard"),
            P(),
        ),
        check_vma=False,
    )
```

```python
import functools

import jax
import jax.numpy as jnp
from jax import lax
from jax.experimental import pallas as pl
from jax.experimental.pallas import tpu as pltpu
from jax.sharding import PartitionSpec as P

MESH = pl.DeviceIdType.MESH
SLOTS = 6
EARLY = ((0, 0), (1, 1), (2, 2), (3, 0), (2, 1), (3, 2))
SOON = 3


def exchange(
    n, groups, late, gate, up, down, weight, gain,
    out_gate, out_up, out_down, scale_gate, scale_up, scale_down, out_router, later,
    in_gate, in_up, in_down, send_gate, send_up, send_down, raw_wide, raw_down,
    part, arrived, mine, crossed, owned, inverse, narrow_router,
    load_sem, half_send, half_recv, cross_send, cross_recv, inv_send, inv_recv,
    big_send, big_recv, own_sem, later_sem, raw_send, raw_recv, raw_out, router_sem,
):
    experts, rows, width = gate.shape
    cols = width // n
    inner = down.shape[2]
    half = n // 2
    first_late = experts - late
    lanes = min(128, inner)
    me = lax.axis_index("shard")
    grp = lax.axis_index("expert")
    side, place = me // half, me % half

    def at(across, step):
        there = lax.rem(side + across, 2)
        q = lax.rem(place + step, half)
        return there, q, there * half + q

    order = []
    for r in range(half):
        order.append((1, r))
        if half - 1 - r > 0:
            order.append((0, half - 1 - r))

    def load(t):
        slot = lax.rem(t, SLOTS)
        return [
            pltpu.make_async_copy(src.at[t], dst.at[slot], load_sem.at[slot, i])
            for i, (src, dst) in enumerate(((gate, in_gate), (up, in_up), (down, in_down)))
        ]

    for copy in load(0):
        copy.start()

    barrier = pltpu.get_barrier_semaphore()
    for k in range(1, n):
        pl.semaphore_signal(
            barrier, inc=1, device_id={"shard": lax.rem(me + k, n)}, device_id_type=MESH
        )
    for k in range(1, groups):
        pl.semaphore_signal(
            barrier, inc=1, device_id={"expert": lax.rem(grp + k, groups)}, device_id_type=MESH
        )

    w = weight[...]
    experts_here, depth = w.shape
    narrow_router[...] = (w * gain[...]).astype(jnp.bfloat16)
    router_rows = pl.ds(pl.multiple_of(grp * experts_here, experts_here), experts_here)

    def router_block(d):
        return out_router.at[router_rows, pl.ds(pl.multiple_of(d * depth, depth), depth)]

    row_at = pl.ds(pl.multiple_of(me * rows, rows), rows)
    col_at = pl.ds(pl.multiple_of(me * inner, inner), inner)

    def router_first(across, step, sem):
        return pltpu.make_async_remote_copy(
            src_ref=narrow_router,
            dst_ref=router_block(me),
            send_sem=router_sem.at[0],
            recv_sem=router_sem.at[sem],
            device_id={"shard": at(across, step)[2]},
            device_id_type=MESH,
        )

    router_own = pltpu.make_async_copy(narrow_router, router_block(me), router_sem.at[2])

    def router_relay(step):
        across = router_block(at(1, 0)[2])
        return pltpu.make_async_remote_copy(
            src_ref=across,
            dst_ref=across,
            send_sem=router_sem.at[0],
            recv_sem=router_sem.at[1],
            device_id={"shard": at(0, step)[2]},
            device_id_type=MESH,
        )

    def router_second(k):
        return pltpu.make_async_remote_copy(
            src_ref=out_router.at[router_rows, :],
            dst_ref=out_router.at[router_rows, :],
            send_sem=router_sem.at[3],
            recv_sem=router_sem.at[4],
            device_id={"expert": lax.rem(grp + k, groups)},
            device_id_type=MESH,
        )

    def block_of(ref, slot, d):
        return ref[slot, :, pl.ds(pl.multiple_of(d * cols, cols), cols)]

    def raw_copy(j):
        r, i = EARLY[j]
        d = at(1, r)[2]
        return pltpu.make_async_remote_copy(
            src_ref=(send_gate, send_up, send_down)[i].at[d],
            dst_ref=raw_down.at[j] if i == 2 else raw_wide.at[j],
            send_sem=raw_send.at[j],
            recv_sem=raw_recv.at[j],
            device_id={"shard": d},
            device_id_type=MESH,
        )

    def raw_fill(j):
        r, i = EARLY[j]
        d = at(1, r)[2]
        if i == 2:
            x = in_down[0, pl.ds(pl.multiple_of(d * cols, cols), cols), :]
        else:
            x = block_of((in_gate, in_up)[i], 0, d)
        (send_gate, send_up, send_down)[i][d] = x.astype(jnp.bfloat16)

    def down_factor(q, h, t):
        return jnp.broadcast_to(inverse[t, q, h, 2], (lanes, cols)).T

    def raw_out_copy(j):
        r, i = EARLY[j]
        s = at(1, half - r)[2]
        if i == 2:
            to = out_down.at[0, :, pl.ds(pl.multiple_of(s * inner, inner), inner)]
            return pltpu.make_async_copy(raw_down.at[j], to, raw_out.at[j])
        to = (out_gate, out_up)[i].at[0, pl.ds(pl.multiple_of(s * rows, rows), rows), :]
        return pltpu.make_async_copy(raw_wide.at[j], to, raw_out.at[j])

    def raw_scale(j):
        _, i = EARLY[j]
        raw_copy(j).wait_recv()
        if i == 2:
            factor = down_factor(place, side, 0)
            for c in range(0, inner, lanes):
                x = raw_down[j, :, c:c + lanes].astype(jnp.float32)
                raw_down[j, :, c:c + lanes] = (x * factor).astype(jnp.bfloat16)
        else:
            x = raw_wide[j].astype(jnp.float32)
            raw_wide[j] = (x * inverse[0, place, side, i]).astype(jnp.bfloat16)

    def sums(t):
        slot = lax.rem(t, SLOTS)
        for d in range(n):
            h, q = d // half, d % half
            for i, ref in enumerate((in_gate, in_up)):
                x = ref[slot, :, d * cols:(d + 1) * cols]
                part[t, q, h, i] = jnp.sum(x * x, axis=0, keepdims=True)
            x = in_down[slot, d * cols:(d + 1) * cols, :]
            x = x * x
            folded = x[:, :lanes]
            for c in range(lanes, inner, lanes):
                folded = folded + x[:, c:c + lanes]
            part[t, q, h, 2] = jnp.sum(folded.T, axis=0, keepdims=True)

    def share(t):
        for k in range(1, half):
            _, q, d = at(0, k)
            pltpu.make_async_remote_copy(
                src_ref=part.at[t, q],
                dst_ref=arrived.at[t, k - 1],
                send_sem=half_send,
                recv_sem=half_recv.at[t],
                device_id={"shard": d},
                device_id_type=MESH,
            ).start()

    def cross_copy(t):
        return pltpu.make_async_remote_copy(
            src_ref=mine.at[t],
            dst_ref=crossed.at[t],
            send_sem=cross_send,
            recv_sem=cross_recv.at[t],
            device_id={"shard": at(1, 0)[2]},
            device_id_type=MESH,
        )

    def cross(t):
        pltpu.make_async_copy(arrived.at[t], arrived.at[t], half_recv.at[t]).wait()
        total = part[t, place]
        for k in range(half - 1):
            total = total + arrived[t, k]
        mine[t] = total
        cross_copy(t).start()

    def reduce(t):
        cross_copy(t).wait_recv()
        for i, out in enumerate((scale_gate, scale_up, scale_down)):
            out[pl.ds(t, 1), :] = jnp.sqrt(mine[t, side, i] + crossed[t, side, i])
        scaled = 1.0 / jnp.sqrt(mine[t] + crossed[t])
        owned[t] = scaled
        inverse[t, place] = scaled
        for k in range(1, half):
            pltpu.make_async_remote_copy(
                src_ref=owned.at[t],
                dst_ref=inverse.at[t, place],
                send_sem=inv_send,
                recv_sem=inv_recv.at[t],
                device_id={"shard": at(0, k)[2]},
                device_id_type=MESH,
            ).start()

    def finish(t, first):
        others = pl.ds(0, half - 1)
        pltpu.make_async_copy(
            inverse.at[t, others], inverse.at[t, others], inv_recv.at[t]
        ).wait()
        slot = lax.rem(t, SLOTS)
        for i, (ref, send, place_at) in enumerate((
            (in_gate, send_gate, out_gate.at[t, row_at, :]),
            (in_up, send_up, out_up.at[t, row_at, :]),
            (in_down, send_down, out_down.at[t, :, col_at]),
        )):
            waiting = None
            for across, step in order + [(0, 0)]:
                if first and across == 1 and (step, i) in EARLY:
                    continue
                h, q, d = at(across, step)
                to = t * n + d
                if i == 2:
                    factor = down_factor(q, h, t)
                    for c in range(0, inner, lanes):
                        x = ref[slot, pl.ds(pl.multiple_of(d * cols, cols), cols), c:c + lanes]
                        send[to, :, c:c + lanes] = (x * factor).astype(jnp.bfloat16)
                else:
                    x = block_of(ref, slot, d)
                    send[to] = (x * inverse[t, q, h, i]).astype(jnp.bfloat16)
                if waiting is not None:
                    waiting()

                def go(across=across, step=step, d=d, to=to):
                    if (across, step) == (0, 0):
                        pltpu.make_async_copy(send.at[to], place_at, own_sem.at[i]).start()
                        return
                    copy = pltpu.make_async_remote_copy(
                        src_ref=send.at[to],
                        dst_ref=place_at,
                        send_sem=big_send.at[i],
                        recv_sem=big_recv.at[i],
                        device_id={"shard": d},
                        device_id_type=MESH,
                    )
                    if i == 2 and (across, step) == (1, half // 2) and not first:
                        @pl.when(t < first_late)
                        def _():
                            copy.start()

                        @pl.when(t >= first_late)
                        def _():
                            pltpu.make_async_copy(
                                send.at[to], later.at[t - first_late], later_sem
                            ).start()
                    else:
                        copy.start()

                waiting = go
            waiting()

    def step(t, carry):
        @pl.when(t + 2 < experts)
        def _():
            for copy in load(t + 2):
                copy.start()

        @pl.when(t < experts)
        def _():
            for copy in load(t):
                copy.wait()
            sums(t)
            share(t)

        @pl.when((t >= 1) & (t <= experts))
        def _():
            cross(t - 1)

        @pl.when(t == 2)
        def _():
            for j in range(SOON, len(EARLY)):
                raw_copy(j).start()

        @pl.when((t >= 2) & (t <= experts + 1))
        def _():
            reduce(t - 2)

        @pl.when(t == 3)
        def _():
            router_first(1, 0, 5).wait_recv()
            for k in range(1, half):
                router_relay(k).start()
            finish(0, True)
            for j in range(len(EARLY)):
                raw_scale(j)
                if j:
                    raw_out_copy(j - 1).start()
            raw_out_copy(len(EARLY) - 1).start()

        @pl.when(t > 3)
        def _():
            finish(t - 3, False)

        return carry

    for copy in load(0):
        copy.wait()
    for t in range(1, 3):
        for copy in load(t):
            copy.start()
    sums(0)
    for j in range(SOON):
        raw_fill(j)
    pl.semaphore_wait(barrier, n - 1 + groups - 1)
    share(0)
    for j in range(SOON):
        raw_copy(j).start()
    router_own.start()
    for k in range(1, half):
        router_first(0, k, 1).start()
    router_first(1, 0, 5).start()
    for j in range(SOON, len(EARLY)):
        raw_fill(j)
    lax.fori_loop(1, experts + 3, step, 0)

    gathered = out_router.at[router_rows, pl.ds(0, (n - 1) * depth)]
    near = out_router.at[router_rows, pl.ds(0, (n - 2) * depth)]
    router_own.wait()
    pltpu.make_async_copy(near, near, router_sem.at[1]).wait()
    for k in range(1, groups):
        router_second(k).start()

    pltpu.make_async_copy(later, later, later_sem).wait()
    for j in range(len(EARLY)):
        raw_copy(j).wait_send()
        raw_out_copy(j).wait()
    for i, send in enumerate((send_gate, send_up, send_down)):
        sent = experts * (n - 1) - sum(j == i for _, j in EARLY)
        if i == 2:
            sent -= late
        blocks = send.at[pl.ds(0, sent)]
        pltpu.make_async_copy(blocks, blocks, big_recv.at[i]).wait()
        pltpu.make_async_copy(blocks, blocks, big_send.at[i]).wait()
        kept = send.at[pl.ds(0, experts)]
        pltpu.make_async_copy(kept, kept, own_sem.at[i]).wait()
    pltpu.make_async_copy(arrived, arrived, half_send).wait()
    pltpu.make_async_copy(crossed, crossed, cross_send).wait()
    others = pl.ds(0, half - 1)
    pltpu.make_async_copy(inverse.at[:, others], inverse.at[:, others], inv_send).wait()
    pltpu.make_async_copy(gathered, gathered, router_sem.at[0]).wait()
    handed = out_router.at[pl.ds(0, (groups - 1) * experts_here), :]
    pltpu.make_async_copy(handed, handed, router_sem.at[3]).wait()
    pltpu.make_async_copy(handed, handed, router_sem.at[4]).wait()


def by_collectives(master_gate, master_up, master_down, router_weight, router_gain):
    total_gate, total_up, total_down = lax.psum(
        (
            jnp.sum(master_gate * master_gate, axis=1),
            jnp.sum(master_up * master_up, axis=1),
            jnp.sum(master_down * master_down, axis=2),
        ),
        "shard",
    )
    scale_gate = jnp.sqrt(total_gate)
    scale_up = jnp.sqrt(total_up)
    scale_down = jnp.sqrt(total_down)
    narrow_gate, narrow_up, narrow_down = (
        (master_gate / jnp.expand_dims(scale_gate, 1)).astype(jnp.bfloat16),
        (master_up / jnp.expand_dims(scale_up, 1)).astype(jnp.bfloat16),
        (master_down / jnp.expand_dims(scale_down, 2)).astype(jnp.bfloat16),
    )
    final_gate, final_up = (
        lax.all_to_all(narrow_gate, "shard", split_axis=2, concat_axis=1, tiled=True),
        lax.all_to_all(narrow_up, "shard", split_axis=2, concat_axis=1, tiled=True),
    )
    final_down = lax.all_to_all(narrow_down, "shard", split_axis=1, concat_axis=2, tiled=True)
    scale_gate = lax.dynamic_slice_in_dim(
        scale_gate, lax.axis_index("shard") * final_gate.shape[2], final_gate.shape[2], axis=1
    )
    scale_up = lax.dynamic_slice_in_dim(
        scale_up, lax.axis_index("shard") * final_up.shape[2], final_up.shape[2], axis=1
    )
    scale_down = lax.dynamic_slice_in_dim(
        scale_down, lax.axis_index("shard") * final_down.shape[1], final_down.shape[1], axis=1
    )
    part_router = (router_weight * router_gain[:, None]).astype(jnp.bfloat16)
    row_router = lax.all_gather(part_router, "shard", axis=0, tiled=True)
    serve_router = lax.all_gather(row_router, "expert", axis=1, tiled=True)
    return (final_gate, final_up, final_down, scale_gate, scale_up, scale_down, serve_router)


def on_device(n, groups, gate, up, down, router_weight, router_gain):
    experts, rows, width = gate.shape
    cols = width // n
    inner = down.shape[2]
    depth, experts_here = router_weight.shape
    if cols % 128 or inner % 128 or depth % 128 or n % 2 or n < 8 or experts < 8:
        return by_collectives(gate, up, down, router_weight, router_gain)
    narrow, wide = jnp.bfloat16, jnp.float32
    half = n // 2
    late = experts * 8 // 16
    dma = pltpu.SemaphoreType.DMA
    any_space = pl.BlockSpec(memory_space=pl.ANY)
    vmem = pl.BlockSpec(memory_space=pltpu.VMEM)
    outs = pl.pallas_call(
        functools.partial(exchange, n, groups, late),
        out_shape=(
            jax.ShapeDtypeStruct((experts, rows * n, cols), narrow),
            jax.ShapeDtypeStruct((experts, rows * n, cols), narrow),
            jax.ShapeDtypeStruct((experts, cols, inner * n), narrow),
            jax.ShapeDtypeStruct((experts, cols), wide),
            jax.ShapeDtypeStruct((experts, cols), wide),
            jax.ShapeDtypeStruct((experts, cols), wide),
            jax.ShapeDtypeStruct((experts_here * groups, depth * n), narrow),
            jax.ShapeDtypeStruct((late, cols, inner), narrow),
        ),
        in_specs=[any_space] * 3 + [vmem] * 2,
        out_specs=(any_space,) * 3 + (vmem,) * 3 + (any_space,) * 2,
        scratch_shapes=[
            pltpu.VMEM((SLOTS, rows, width), wide),
            pltpu.VMEM((SLOTS, rows, width), wide),
            pltpu.VMEM((SLOTS, width, inner), wide),
            pltpu.VMEM((experts * n, rows, cols), narrow),
            pltpu.VMEM((experts * n, rows, cols), narrow),
            pltpu.VMEM((experts * n, cols, inner), narrow),
            pltpu.VMEM((len(EARLY), rows, cols), narrow),
            pltpu.VMEM((len(EARLY), cols, inner), narrow),
            pltpu.VMEM((experts, half, 2, 3, 1, cols), wide),
            pltpu.VMEM((experts, half - 1, 2, 3, 1, cols), wide),
            pltpu.VMEM((experts, 2, 3, 1, cols), wide),
            pltpu.VMEM((experts, 2, 3, 1, cols), wide),
            pltpu.VMEM((experts, 2, 3, 1, cols), wide),
            pltpu.VMEM((experts, half, 2, 3, 1, cols), wide),
            pltpu.VMEM((experts_here, depth), narrow),
            dma((SLOTS, 3)),
            dma,
            dma((experts,)),
            dma,
            dma((experts,)),
            dma,
            dma((experts,)),
            dma((3,)),
            dma((3,)),
            dma((3,)),
            dma,
            dma((len(EARLY),)),
            dma((len(EARLY),)),
            dma((len(EARLY),)),
            dma((6,)),
        ],
        compiler_params=pltpu.CompilerParams(
            collective_id=0, has_side_effects=True, vmem_limit_bytes=60 * 2**20
        ),
    )(gate, up, down, router_weight.T, router_gain[None, :])
    swap = [(d, n - half * (d // half + 1) + (d + half // 2) % half) for d in range(n)]
    late_blocks = lax.ppermute(outs[7], "shard", swap)

    big = [jax.ShapeDtypeStruct(x.shape, x.dtype) for x in outs[:3]]
    small = [jax.ShapeDtypeStruct(x.shape, x.dtype) for x in outs[3:7]]
    moved = sum(x.size * x.dtype.itemsize for x in outs[:7])
    placed = pl.pallas_call(
        place,
        in_specs=[any_space] * 3 + [vmem] * 4,
        out_specs=[any_space] * 3 + [vmem] * 4,
        out_shape=big + small,
        scratch_shapes=[pltpu.VMEM(x.shape, x.dtype) for x in big]
        + [dma((3, experts)), dma((3, experts))],
        compiler_params=pltpu.CompilerParams(vmem_limit_bytes=60 * 2**20),
        cost_estimate=pl.CostEstimate(flops=0, bytes_accessed=2 * moved, transcendentals=0),
    )(*outs[:7])
    final_down = pl.pallas_call(
        functools.partial(place_late, n),
        in_specs=[any_space] * 2,
        out_specs=any_space,
        out_shape=jax.ShapeDtypeStruct(outs[2].shape, narrow),
        input_output_aliases={0: 0},
        scratch_shapes=[dma],
        compiler_params=pltpu.CompilerParams(vmem_limit_bytes=2**20),
    )(placed[2], late_blocks)
    return tuple(placed[:2]) + (final_down,) + tuple(placed[3:6]) + (placed[6].T,)


def place(*refs):
    srcs, dsts, held, taken, given = refs[:7], refs[7:14], refs[14:17], refs[17], refs[18]
    pairs = [(t, i) for t in range(srcs[0].shape[0]) for i in range(3)]

    def take(t, i):
        return pltpu.make_async_copy(srcs[i].at[t], held[i].at[t], taken.at[i, t])

    def give(t, i):
        return pltpu.make_async_copy(held[i].at[t], dsts[i].at[t], given.at[i, t])

    for t, i in pairs:
        take(t, i).start()
    for src, dst in zip(srcs[3:], dsts[3:]):
        dst[...] = src[...]
    for t, i in pairs:
        take(t, i).wait()
        give(t, i).start()
    for t, i in pairs:
        give(t, i).wait()


def place_late(n, _, late, out, sem):
    count, _, inner = late.shape
    me, half = lax.axis_index("shard"), n // 2
    source = (1 - me // half) * half + lax.rem(me + half // 2, half)
    cols = pl.ds(pl.multiple_of(source * inner, inner), inner)
    copy = pltpu.make_async_copy(
        late, out.at[pl.ds(out.shape[0] - count, count), :, cols], sem
    )
    copy.start()
    copy.wait()


def solution(mesh):
    placed = (
        P("expert", "shard", None),
        P("expert", "shard", None),
        P("expert", None, "shard"),
        P("shard", "expert"),
        P("shard"),
    )
    return jax.shard_map(
        functools.partial(on_device, mesh.shape["shard"], mesh.shape["expert"]),
        mesh=mesh,
        in_specs=placed,
        out_specs=(
            P("expert", None, "shard"),
            P("expert", None, "shard"),
            P("expert", "shard", None),
            P("expert", "shard"),
            P("expert", "shard"),
            P("expert", "shard"),
            P(),
        ),
        check_vma=False,
    )
```

```python
import functools

import jax
import jax.numpy as jnp
from jax import lax
from jax.experimental import pallas as pl
from jax.experimental.pallas import tpu as pltpu
from jax.sharding import PartitionSpec as P

MESH = pl.DeviceIdType.MESH
SLOTS = 6
HELD = 2
EARLY = ((0, 0), (1, 1), (2, 2), (3, 0), (2, 1), (3, 2))
SOON = 3


def exchange(
    n, groups, late, late_outer, gate, up, down, weight, gain,
    out_gate, out_up, out_down, scale_gate, scale_up, scale_down, out_router, later, later_outer,
    in_gate, in_up, in_down, send_gate, send_up, send_down, raw_wide, raw_down,
    part, arrived, mine, crossed, owned, inverse, narrow_router,
    load_sem, half_send, half_recv, cross_send, cross_recv, inv_send, inv_recv,
    big_send, big_recv, own_sem, later_sem, raw_send, raw_recv, raw_out, router_sem,
):
    experts, rows, width = gate.shape
    cols = width // n
    inner = down.shape[2]
    half = n // 2
    first_late = experts - late
    first_outer = experts - late_outer
    lanes = min(128, inner)
    me = lax.axis_index("shard")
    grp = lax.axis_index("expert")
    side, place = me // half, me % half
    inner_one = side + place // (half // 2) == 1

    def at(across, step):
        there = lax.rem(side + across, 2)
        q = lax.rem(place + step, half)
        return there, q, there * half + q

    order = []
    for r in range(half):
        order.append((1, r))
        if half - 1 - r > 0:
            order.append((0, half - 1 - r))

    def load(t):
        slot = lax.rem(t, SLOTS)
        return [
            pltpu.make_async_copy(src.at[t], dst.at[slot], load_sem.at[slot, i])
            for i, (src, dst) in enumerate(((gate, in_gate), (up, in_up), (down, in_down)))
        ]

    for copy in load(0):
        copy.start()

    barrier = pltpu.get_barrier_semaphore()
    for k in range(1, n):
        pl.semaphore_signal(
            barrier, inc=1, device_id={"shard": lax.rem(me + k, n)}, device_id_type=MESH
        )
    for k in range(1, groups):
        pl.semaphore_signal(
            barrier, inc=1, device_id={"expert": lax.rem(grp + k, groups)}, device_id_type=MESH
        )

    w = weight[...]
    experts_here, depth = w.shape
    narrow_router[...] = (w * gain[...]).astype(jnp.bfloat16)
    router_rows = pl.ds(pl.multiple_of(grp * experts_here, experts_here), experts_here)

    def router_block(d):
        return out_router.at[router_rows, pl.ds(pl.multiple_of(d * depth, depth), depth)]

    row_at = pl.ds(pl.multiple_of(me * rows, rows), rows)
    col_at = pl.ds(pl.multiple_of(me * inner, inner), inner)

    def router_first(across, step, sem):
        return pltpu.make_async_remote_copy(
            src_ref=narrow_router,
            dst_ref=router_block(me),
            send_sem=router_sem.at[0],
            recv_sem=router_sem.at[sem],
            device_id={"shard": at(across, step)[2]},
            device_id_type=MESH,
        )

    router_own = pltpu.make_async_copy(narrow_router, router_block(me), router_sem.at[2])

    def router_relay(step):
        across = router_block(at(1, 0)[2])
        return pltpu.make_async_remote_copy(
            src_ref=across,
            dst_ref=across,
            send_sem=router_sem.at[0],
            recv_sem=router_sem.at[1],
            device_id={"shard": at(0, step)[2]},
            device_id_type=MESH,
        )

    def router_second(k):
        return pltpu.make_async_remote_copy(
            src_ref=out_router.at[router_rows, :],
            dst_ref=out_router.at[router_rows, :],
            send_sem=router_sem.at[3],
            recv_sem=router_sem.at[4],
            device_id={"expert": lax.rem(grp + k, groups)},
            device_id_type=MESH,
        )

    def block_of(ref, slot, d):
        return ref[slot, :, pl.ds(pl.multiple_of(d * cols, cols), cols)]

    def raw_copy(j):
        r, i = EARLY[j]
        d = at(1, r)[2]
        return pltpu.make_async_remote_copy(
            src_ref=(send_gate, send_up, send_down)[i].at[d],
            dst_ref=raw_down.at[j] if i == 2 else raw_wide.at[j],
            send_sem=raw_send.at[j],
            recv_sem=raw_recv.at[j],
            device_id={"shard": d},
            device_id_type=MESH,
        )

    def raw_fill(j):
        r, i = EARLY[j]
        d = at(1, r)[2]
        if i == 2:
            x = in_down[0, pl.ds(pl.multiple_of(d * cols, cols), cols), :]
        else:
            x = block_of((in_gate, in_up)[i], 0, d)
        (send_gate, send_up, send_down)[i][d] = x.astype(jnp.bfloat16)

    def down_factor(q, h, t):
        return jnp.broadcast_to(inverse[t, q, h, 2], (lanes, cols)).T

    def raw_out_copy(j):
        r, i = EARLY[j]
        s = at(1, half - r)[2]
        if i == 2:
            to = out_down.at[0, :, pl.ds(pl.multiple_of(s * inner, inner), inner)]
            return pltpu.make_async_copy(raw_down.at[j], to, raw_out.at[j])
        to = (out_gate, out_up)[i].at[0, pl.ds(pl.multiple_of(s * rows, rows), rows), :]
        return pltpu.make_async_copy(raw_wide.at[j], to, raw_out.at[j])

    def raw_scale(j):
        _, i = EARLY[j]
        raw_copy(j).wait_recv()
        if i == 2:
            factor = down_factor(place, side, 0)
            for c in range(0, inner, lanes):
                x = raw_down[j, :, c:c + lanes].astype(jnp.float32)
                raw_down[j, :, c:c + lanes] = (x * factor).astype(jnp.bfloat16)
        else:
            x = raw_wide[j].astype(jnp.float32)
            raw_wide[j] = (x * inverse[0, place, side, i]).astype(jnp.bfloat16)

    def sums(t):
        slot = lax.rem(t, SLOTS)
        for d in range(n):
            h, q = d // half, d % half
            for i, ref in enumerate((in_gate, in_up)):
                x = ref[slot, :, d * cols:(d + 1) * cols]
                part[t, q, h, i] = jnp.sum(x * x, axis=0, keepdims=True)
            x = in_down[slot, d * cols:(d + 1) * cols, :]
            x = x * x
            folded = x[:, :lanes]
            for c in range(lanes, inner, lanes):
                folded = folded + x[:, c:c + lanes]
            part[t, q, h, 2] = jnp.sum(folded.T, axis=0, keepdims=True)

    def share(t):
        for k in range(1, half):
            _, q, d = at(0, k)
            pltpu.make_async_remote_copy(
                src_ref=part.at[t, q],
                dst_ref=arrived.at[t, k - 1],
                send_sem=half_send,
                recv_sem=half_recv.at[t],
                device_id={"shard": d},
                device_id_type=MESH,
            ).start()

    def cross_copy(t):
        return pltpu.make_async_remote_copy(
            src_ref=mine.at[t],
            dst_ref=crossed.at[t],
            send_sem=cross_send,
            recv_sem=cross_recv.at[t],
            device_id={"shard": at(1, 0)[2]},
            device_id_type=MESH,
        )

    def cross(t):
        pltpu.make_async_copy(arrived.at[t], arrived.at[t], half_recv.at[t]).wait()
        total = part[t, place]
        for k in range(half - 1):
            total = total + arrived[t, k]
        mine[t] = total
        cross_copy(t).start()

    def reduce(t):
        cross_copy(t).wait_recv()
        for i, out in enumerate((scale_gate, scale_up, scale_down)):
            out[pl.ds(t, 1), :] = jnp.sqrt(mine[t, side, i] + crossed[t, side, i])
        scaled = 1.0 / jnp.sqrt(mine[t] + crossed[t])
        owned[t] = scaled
        inverse[t, place] = scaled
        for k in range(1, half):
            pltpu.make_async_remote_copy(
                src_ref=owned.at[t],
                dst_ref=inverse.at[t, place],
                send_sem=inv_send,
                recv_sem=inv_recv.at[t],
                device_id={"shard": at(0, k)[2]},
                device_id_type=MESH,
            ).start()

    def finish(t, first):
        others = pl.ds(0, half - 1)
        pltpu.make_async_copy(
            inverse.at[t, others], inverse.at[t, others], inv_recv.at[t]
        ).wait()
        slot = lax.rem(t, SLOTS)
        for i, (ref, send, place_at) in enumerate((
            (in_gate, send_gate, out_gate.at[t, row_at, :]),
            (in_up, send_up, out_up.at[t, row_at, :]),
            (in_down, send_down, out_down.at[t, :, col_at]),
        )):
            waiting = None
            for across, step in order + [(0, 0)]:
                if first and across == 1 and (step, i) in EARLY:
                    continue
                h, q, d = at(across, step)
                to = t * n + d
                if i == 2:
                    factor = down_factor(q, h, t)
                    for c in range(0, inner, lanes):
                        x = ref[slot, pl.ds(pl.multiple_of(d * cols, cols), cols), c:c + lanes]
                        send[to, :, c:c + lanes] = (x * factor).astype(jnp.bfloat16)
                else:
                    x = block_of(ref, slot, d)
                    send[to] = (x * inverse[t, q, h, i]).astype(jnp.bfloat16)
                if waiting is not None:
                    waiting()

                def go(across=across, step=step, d=d, to=to):
                    if (across, step) == (0, 0):
                        pltpu.make_async_copy(send.at[to], place_at, own_sem.at[i]).start()
                        return
                    copy = pltpu.make_async_remote_copy(
                        src_ref=send.at[to],
                        dst_ref=place_at,
                        send_sem=big_send.at[i],
                        recv_sem=big_recv.at[i],
                        device_id={"shard": d},
                        device_id_type=MESH,
                    )
                    if i < 2 and (across, step) == (1, half // 2) and not first:
                        @pl.when(jnp.logical_not(inner_one & (t >= experts - HELD)))
                        def _():
                            copy.start()
                    elif i == 2 and (across, step) == (1, half // 2) and not first:
                        kept = inner_one & (t >= first_late)
                        kept_outer = jnp.logical_not(inner_one) & (t >= first_outer)

                        @pl.when(jnp.logical_not(kept | kept_outer))
                        def _():
                            copy.start()

                        @pl.when(kept)
                        def _():
                            pltpu.make_async_copy(
                                send.at[to], later.at[t - first_late], later_sem
                            ).start()

                        @pl.when(kept_outer)
                        def _():
                            pltpu.make_async_copy(
                                send.at[to], later_outer.at[t - first_outer], later_sem
                            ).start()
                    else:
                        copy.start()

                waiting = go
            waiting()

    def send_held():
        d = at(1, half // 2)[2]
        for t in range(experts - HELD, experts):
            for i, (send, out) in enumerate(((send_gate, out_gate), (send_up, out_up))):
                pltpu.make_async_remote_copy(
                    src_ref=send.at[t * n + d],
                    dst_ref=out.at[t, row_at, :],
                    send_sem=big_send.at[i],
                    recv_sem=big_recv.at[i],
                    device_id={"shard": d},
                    device_id_type=MESH,
                ).start()

    def step(t, carry):
        @pl.when(t + 2 < experts)
        def _():
            for copy in load(t + 2):
                copy.start()

        @pl.when(t < experts)
        def _():
            for copy in load(t):
                copy.wait()
            sums(t)
            share(t)

        @pl.when((t >= 1) & (t <= experts))
        def _():
            cross(t - 1)

        @pl.when(t == 2)
        def _():
            for j in range(SOON, len(EARLY)):
                raw_copy(j).start()

        @pl.when((t >= 2) & (t <= experts + 1))
        def _():
            reduce(t - 2)

        @pl.when(t == 3)
        def _():
            router_first(1, 0, 5).wait_recv()
            for k in range(1, half):
                router_relay(k).start()
            finish(0, True)
            for j in range(len(EARLY)):
                raw_scale(j)
                if j:
                    raw_out_copy(j - 1).start()
            raw_out_copy(len(EARLY) - 1).start()

        @pl.when(t > 3)
        def _():
            finish(t - 3, False)

        return carry

    for copy in load(0):
        copy.wait()
    for t in range(1, 3):
        for copy in load(t):
            copy.start()
    sums(0)
    for j in range(SOON):
        raw_fill(j)
    pl.semaphore_wait(barrier, n - 1 + groups - 1)
    share(0)
    for j in range(SOON):
        raw_copy(j).start()
    router_own.start()
    for k in range(1, half):
        router_first(0, k, 1).start()
    router_first(1, 0, 5).start()
    for j in range(SOON, len(EARLY)):
        raw_fill(j)
    lax.fori_loop(1, experts + 3, step, 0)

    pl.when(inner_one)(send_held)

    gathered = out_router.at[router_rows, pl.ds(0, (n - 1) * depth)]
    near = out_router.at[router_rows, pl.ds(0, (n - 2) * depth)]
    router_own.wait()
    pltpu.make_async_copy(near, near, router_sem.at[1]).wait()
    for k in range(1, groups):
        router_second(k).start()

    for j in range(len(EARLY)):
        raw_copy(j).wait_send()
        raw_out_copy(j).wait()
    for i, send in enumerate((send_gate, send_up, send_down)):
        sent = experts * (n - 1) - sum(j == i for _, j in EARLY)

        def landed(sent, i=i, send=send):
            blocks = send.at[pl.ds(0, sent)]
            pltpu.make_async_copy(blocks, blocks, big_recv.at[i]).wait()
            pltpu.make_async_copy(blocks, blocks, big_send.at[i]).wait()

        if i == 2:
            for those, buffer, count in (
                (inner_one, later, late),
                (jnp.logical_not(inner_one), later_outer, late_outer),
            ):
                @pl.when(those)
                def _(buffer=buffer, count=count, sent=sent, landed=landed):
                    pltpu.make_async_copy(buffer, buffer, later_sem).wait()
                    landed(sent - count)
        else:
            landed(sent)
        kept = send.at[pl.ds(0, experts)]
        pltpu.make_async_copy(kept, kept, own_sem.at[i]).wait()
    pltpu.make_async_copy(arrived, arrived, half_send).wait()
    pltpu.make_async_copy(crossed, crossed, cross_send).wait()
    others = pl.ds(0, half - 1)
    pltpu.make_async_copy(inverse.at[:, others], inverse.at[:, others], inv_send).wait()
    pltpu.make_async_copy(gathered, gathered, router_sem.at[0]).wait()
    handed = out_router.at[pl.ds(0, (groups - 1) * experts_here), :]
    pltpu.make_async_copy(handed, handed, router_sem.at[3]).wait()
    pltpu.make_async_copy(handed, handed, router_sem.at[4]).wait()


def by_collectives(master_gate, master_up, master_down, router_weight, router_gain):
    total_gate, total_up, total_down = lax.psum(
        (
            jnp.sum(master_gate * master_gate, axis=1),
            jnp.sum(master_up * master_up, axis=1),
            jnp.sum(master_down * master_down, axis=2),
        ),
        "shard",
    )
    scale_gate = jnp.sqrt(total_gate)
    scale_up = jnp.sqrt(total_up)
    scale_down = jnp.sqrt(total_down)
    narrow_gate, narrow_up, narrow_down = (
        (master_gate / jnp.expand_dims(scale_gate, 1)).astype(jnp.bfloat16),
        (master_up / jnp.expand_dims(scale_up, 1)).astype(jnp.bfloat16),
        (master_down / jnp.expand_dims(scale_down, 2)).astype(jnp.bfloat16),
    )
    final_gate, final_up = (
        lax.all_to_all(narrow_gate, "shard", split_axis=2, concat_axis=1, tiled=True),
        lax.all_to_all(narrow_up, "shard", split_axis=2, concat_axis=1, tiled=True),
    )
    final_down = lax.all_to_all(narrow_down, "shard", split_axis=1, concat_axis=2, tiled=True)
    scale_gate = lax.dynamic_slice_in_dim(
        scale_gate, lax.axis_index("shard") * final_gate.shape[2], final_gate.shape[2], axis=1
    )
    scale_up = lax.dynamic_slice_in_dim(
        scale_up, lax.axis_index("shard") * final_up.shape[2], final_up.shape[2], axis=1
    )
    scale_down = lax.dynamic_slice_in_dim(
        scale_down, lax.axis_index("shard") * final_down.shape[1], final_down.shape[1], axis=1
    )
    part_router = (router_weight * router_gain[:, None]).astype(jnp.bfloat16)
    row_router = lax.all_gather(part_router, "shard", axis=0, tiled=True)
    serve_router = lax.all_gather(row_router, "expert", axis=1, tiled=True)
    return (final_gate, final_up, final_down, scale_gate, scale_up, scale_down, serve_router)


def on_device(n, groups, gate, up, down, router_weight, router_gain):
    experts, rows, width = gate.shape
    cols = width // n
    inner = down.shape[2]
    depth, experts_here = router_weight.shape
    if cols % 128 or inner % 128 or depth % 128 or n % 4 or n < 8 or experts % 16:
        return by_collectives(gate, up, down, router_weight, router_gain)
    narrow, wide = jnp.bfloat16, jnp.float32
    half = n // 2
    late, late_outer = experts * 12 // 16, experts * 4 // 16
    dma = pltpu.SemaphoreType.DMA
    any_space = pl.BlockSpec(memory_space=pl.ANY)
    vmem = pl.BlockSpec(memory_space=pltpu.VMEM)
    outs = pl.pallas_call(
        functools.partial(exchange, n, groups, late, late_outer),
        out_shape=(
            jax.ShapeDtypeStruct((experts, rows * n, cols), narrow),
            jax.ShapeDtypeStruct((experts, rows * n, cols), narrow),
            jax.ShapeDtypeStruct((experts, cols, inner * n), narrow),
            jax.ShapeDtypeStruct((experts, cols), wide),
            jax.ShapeDtypeStruct((experts, cols), wide),
            jax.ShapeDtypeStruct((experts, cols), wide),
            jax.ShapeDtypeStruct((experts_here * groups, depth * n), narrow),
            jax.ShapeDtypeStruct((late, cols, inner), narrow),
            jax.ShapeDtypeStruct((late_outer, cols, inner), narrow),
        ),
        in_specs=[any_space] * 3 + [vmem] * 2,
        out_specs=(any_space,) * 3 + (vmem,) * 3 + (any_space,) * 3,
        scratch_shapes=[
            pltpu.VMEM((SLOTS, rows, width), wide),
            pltpu.VMEM((SLOTS, rows, width), wide),
            pltpu.VMEM((SLOTS, width, inner), wide),
            pltpu.VMEM((experts * n, rows, cols), narrow),
            pltpu.VMEM((experts * n, rows, cols), narrow),
            pltpu.VMEM((experts * n, cols, inner), narrow),
            pltpu.VMEM((len(EARLY), rows, cols), narrow),
            pltpu.VMEM((len(EARLY), cols, inner), narrow),
            pltpu.VMEM((experts, half, 2, 3, 1, cols), wide),
            pltpu.VMEM((experts, half - 1, 2, 3, 1, cols), wide),
            pltpu.VMEM((experts, 2, 3, 1, cols), wide),
            pltpu.VMEM((experts, 2, 3, 1, cols), wide),
            pltpu.VMEM((experts, 2, 3, 1, cols), wide),
            pltpu.VMEM((experts, half, 2, 3, 1, cols), wide),
            pltpu.VMEM((experts_here, depth), narrow),
            dma((SLOTS, 3)),
            dma,
            dma((experts,)),
            dma,
            dma((experts,)),
            dma,
            dma((experts,)),
            dma((3,)),
            dma((3,)),
            dma((3,)),
            dma,
            dma((len(EARLY),)),
            dma((len(EARLY),)),
            dma((len(EARLY),)),
            dma((6,)),
        ],
        compiler_params=pltpu.CompilerParams(
            collective_id=0, has_side_effects=True, vmem_limit_bytes=60 * 2**20
        ),
    )(gate, up, down, router_weight.T, router_gain[None, :])
    swaps = [[], []]
    for d in range(half):
        to = half + (d + half // 2) % half
        swaps[d < half // 2] += [(d, to), (to, d)]
    late_blocks = lax.ppermute(outs[7], "shard", swaps[0])
    outer_blocks = lax.ppermute(outs[8], "shard", swaps[1])
    big = [jax.ShapeDtypeStruct(x.shape, x.dtype) for x in outs[:3]]
    small = [jax.ShapeDtypeStruct(x.shape, x.dtype) for x in outs[3:7]]
    moved = sum(x.size * x.dtype.itemsize for x in outs[:7])
    placed = pl.pallas_call(
        place,
        in_specs=[any_space] * 3 + [vmem] * 4,
        out_specs=[any_space] * 3 + [vmem] * 4,
        out_shape=big + small,
        scratch_shapes=[pltpu.VMEM(x.shape, x.dtype) for x in big]
        + [dma((3, experts)), dma((3, experts))],
        compiler_params=pltpu.CompilerParams(vmem_limit_bytes=60 * 2**20),
        cost_estimate=pl.CostEstimate(flops=0, bytes_accessed=2 * moved, transcendentals=0),
    )(*outs[:7])
    final_down = pl.pallas_call(
        functools.partial(place_late, n),
        in_specs=[any_space] * 3,
        out_specs=any_space,
        out_shape=jax.ShapeDtypeStruct(outs[2].shape, narrow),
        input_output_aliases={0: 0},
        scratch_shapes=[dma],
        compiler_params=pltpu.CompilerParams(vmem_limit_bytes=2**20),
    )(placed[2], late_blocks, outer_blocks)
    return tuple(placed[:2]) + (final_down,) + tuple(placed[3:6]) + (placed[6].T,)


def place(*refs):
    srcs, dsts, held, taken, given = refs[:7], refs[7:14], refs[14:17], refs[17], refs[18]
    pairs = [(t, i) for t in range(srcs[0].shape[0]) for i in range(3)]

    def take(t, i):
        return pltpu.make_async_copy(srcs[i].at[t], held[i].at[t], taken.at[i, t])

    def give(t, i):
        return pltpu.make_async_copy(held[i].at[t], dsts[i].at[t], given.at[i, t])

    for t, i in pairs:
        take(t, i).start()
    for src, dst in zip(srcs[3:], dsts[3:]):
        dst[...] = src[...]
    for t, i in pairs:
        take(t, i).wait()
        give(t, i).start()
    for t, i in pairs:
        give(t, i).wait()


def place_late(n, _, late, late_outer, out, sem):
    me, half = lax.axis_index("shard"), n // 2
    source = (1 - me // half) * half + lax.rem(me + half // 2, half)
    inner_one = (me >= half // 2) & (me < half + half // 2)
    for those, blocks in ((inner_one, late), (jnp.logical_not(inner_one), late_outer)):
        count, _, inner = blocks.shape
        cols = pl.ds(pl.multiple_of(source * inner, inner), inner)

        @pl.when(those)
        def _(blocks=blocks, count=count, cols=cols):
            copy = pltpu.make_async_copy(
                blocks, out.at[pl.ds(out.shape[0] - count, count), :, cols], sem
            )
            copy.start()
            copy.wait()


def solution(mesh):
    placed = (
        P("expert", "shard", None),
        P("expert", "shard", None),
        P("expert", None, "shard"),
        P("shard", "expert"),
        P("shard"),
    )
    return jax.shard_map(
        functools.partial(on_device, mesh.shape["shard"], mesh.shape["expert"]),
        mesh=mesh,
        in_specs=placed,
        out_specs=(
            P("expert", None, "shard"),
            P("expert", None, "shard"),
            P("expert", "shard", None),
            P("expert", "shard"),
            P("expert", "shard"),
            P("expert", "shard"),
            P(),
        ),
        check_vma=False,
    )
```
